128 devices in a mesh: grp: 4 (over z), tile: 32 (over x, y, core).
Axes of the slice: x: 4, y: 4, z: 4, core: 2. Of those that a mesh axis runs over, the one named last changes fastest.
Arguments:
- noise: bfloat16 [16, 3, 2048, 2048], P('grp', None, 'tile'), may hold values from -6 to 6
- stress: float32 [6, 2048, 2048], P(None, 'tile', 'grp'), as said below
- timescale: float32 [2048, 2048], P('tile', 'grp'), may hold values from 3 to 256
- mean_inflow: float32 [2048, 2048], P('tile', 'grp'), may hold values from 0.5 to 1.5
- courant: float32 [2048, 2048], P('tile', 'grp'), may hold values from 0.2 to 0.9
- prior_state: float32 [3, 2048, 2048], P(None, 'tile', 'grp'), may hold values from -6 to 6
- field: float32 [3, 8, 2048, 2048], P(None, None, 'tile', 'grp'), may hold values from -6 to 6
Outputs:
- inflow: bfloat16 [16, 3, 2048, 2048], P(None, None, 'tile', 'grp')
- field_out: float32 [3, 8, 2048, 2048], P(None, None, 'tile', 'grp')
The draws below stay inside these ranges and needn't reach their ends.
Inputs may be any that keep to these rules, and one draw needn't show every extreme that they name: stress holds, per cell, R11, R21, R22, R31, R32, R33 of a symmetric positive definite tensor whose Cholesky factor has diagonal entries of 0.3 or more.
All inputs are finite; a program needn't handle non-finite values.
Results may differ from the reference program's by a relative error of at most 0.0085.
Values may be sent and summed in bfloat16 or wider, within the bound.
No kernel may reach another device: no remote copies, remote signals or barrier semaphores. Data moves between devices by JAX's collectives and lax.ppermute only.
A program may use at most 128 MiB of HBM per device.

```python
import math
import jax
import jax.numpy as jnp
from jax import lax

NY = 2048
NZ = 2048
LS = 2
FW = 4
CX = 8
PLANES = 16


def draw_stress(key, part):
    diag_key = jax.random.fold_in(key, 11)
    lower_key = jax.random.fold_in(key, 23)
    smallest, largest, reach = (0.3, 1.5, 0.6)
    diagonal = jnp.exp(jax.random.uniform(diag_key, (3, NZ, NY), jnp.float32, math.log(smallest), math.log(largest)))
    lower = jax.random.uniform(lower_key, (3, NZ, NY), jnp.float32, -reach, reach)
    first_diag, second_diag, third_diag = (diagonal[0], diagonal[1], diagonal[2])
    second_low, third_low, third_mid = (lower[0], lower[1], lower[2])
    return jnp.stack([first_diag * first_diag, second_low * first_diag, second_low * second_low + second_diag * second_diag, third_low * first_diag, third_low * second_low + third_mid * second_diag, third_low * third_low + third_mid * third_mid + third_diag * third_diag]).astype(jnp.float32)


def block_scale(key, dims, cuts, low, high):
    loudness, own = 1.0, jax.random.fold_in(key, 6)
    for dim, shards_of in cuts:
        heights = jnp.exp(jax.random.uniform(jax.random.fold_in(own, dim), (shards_of,), jnp.float32, low / len(cuts), high / len(cuts)))
        loudness = loudness * jnp.repeat(heights, dims[dim] // shards_of).reshape([-1 if axis == dim else 1 for axis in range(len(dims))])
    return loudness


def normal_values(own_key, extent, spread, bound, split=(), held_as=jnp.bfloat16):
    result = spread * jax.random.normal(own_key, extent, jnp.float32)
    if split:
        result = result * block_scale(own_key, extent, split, -0.22, 0.18)
    return jnp.clip(result, -bound, bound).astype(held_as)


def setup_inputs(seed: int = 0) -> dict:
    key_of = jax.random.split(jax.random.key(seed), 8)
    noise = normal_values(key_of[0], (PLANES, 3, NY, NZ), 1.0, 6.0, ((0, 4), (2, 32)))
    stress = draw_stress(jax.random.fold_in(key_of[7], 71), 0)
    timescale = jnp.clip(jnp.exp(math.log(256.0) - 4.446565 * jax.random.uniform(key_of[2], (NZ, NY), jnp.float32) ** block_scale(key_of[2], (NZ, NY), ((0, 32), (1, 4)), -0.2, 0.2)), 3.0, 256.0)
    mean_inflow = jnp.clip(0.5 + 1.0 * jax.random.uniform(key_of[3], (NZ, NY), jnp.float32) ** block_scale(key_of[3], (NZ, NY), ((0, 32), (1, 4)), -0.2, 0.2), 0.5, 1.5)
    courant = jnp.clip(jnp.exp(math.log(0.9) - 1.50407736 * jax.random.uniform(key_of[4], (NZ, NY), jnp.float32) ** block_scale(key_of[4], (NZ, NY), ((0, 32), (1, 4)), -0.2, 0.2)), 0.2, 0.9)
    prior_state = normal_values(key_of[5], (3, NZ, NY), 1.0, 6.0, ((1, 32), (2, 4)), jnp.float32)
    field = normal_values(key_of[6], (3, CX, NZ, NY), 1.0, 6.0, ((2, 32), (3, 4)), jnp.float32)
    return dict(noise=noise, stress=stress, timescale=timescale, mean_inflow=mean_inflow, courant=courant, prior_state=prior_state, field=field)


def filter_taps():
    offsets = jnp.arange(-FW, FW + 1).astype(jnp.float32)
    raw = jnp.exp(-math.pi * offsets * offsets / (2.0 * LS * LS))
    return (raw / jnp.sqrt(jnp.sum(raw * raw))).astype(jnp.bfloat16)

def cholesky_cells(stress):
    first_diag = jnp.sqrt(stress[0])
    second_low = stress[1] / first_diag
    second_diag = jnp.sqrt(stress[2] - second_low * second_low)
    third_low = stress[3] / first_diag
    third_mid = (stress[4] - second_low * third_low) / second_diag
    third_diag = jnp.sqrt(stress[5] - third_low * third_low - third_mid * third_mid)
    return (first_diag, second_low, second_diag, third_low, third_mid, third_diag)

def velocity_of(state, factors, mean_inflow):
    first_diag, second_low, second_diag, third_low, third_mid, third_diag = factors
    return jnp.stack([mean_inflow + first_diag * state[0], second_low * state[0] + second_diag * state[1], third_low * state[0] + third_mid * state[1] + third_diag * state[2]])

def march(current, courant, velocity):
    upstream = jnp.concatenate([velocity[:, None], current[:, :-1]], axis=1)
    return (1.0 - courant) * current + courant * upstream

def reference(noise, stress, timescale, mean_inflow, courant, prior_state, field):
    taps = filter_taps().astype(jnp.float32)
    decay = jnp.exp(-math.pi / (2.0 * timescale))
    gain = jnp.sqrt(1.0 - decay * decay)
    factors = cholesky_cells(stress)

    def one_plane(carry, plane):
        state, current = carry
        span = jnp.zeros(plane.shape, jnp.float32)
        for offset in range(2 * FW + 1):
            span = span + taps[offset] * jnp.roll(plane, FW - offset, axis=2).astype(jnp.float32)
        rounded = lax.optimization_barrier(span.astype(jnp.bfloat16))
        padded = jnp.pad(rounded, ((0, 0), (FW, FW), (0, 0))).astype(jnp.float32)
        filtered = jnp.zeros(plane.shape, jnp.float32)
        for offset in range(2 * FW + 1):
            filtered = filtered + taps[offset] * padded[:, offset:offset + NY, :]
        state = decay * state + gain * jnp.swapaxes(filtered, 1, 2)
        velocity = velocity_of(state, factors, mean_inflow)
        current = march(current, courant, velocity)
        return ((state, current), velocity.astype(jnp.bfloat16))
    (state, current), inflow = lax.scan(one_plane, (prior_state, field), noise)
    return (inflow, current)
```

```python
import math

import jax
import jax.numpy as jnp
import ml_dtypes
import numpy as np
from jax import lax
from jax.experimental import pallas as pl
from jax.experimental.pallas import tpu as pltpu
from jax.sharding import PartitionSpec as P

LS = 2
FW = 4
TAPS = 2 * FW + 1
CX = 8
BF16 = jnp.bfloat16
F32 = jnp.float32


def filter_taps():
    offsets = np.arange(-FW, FW + 1, dtype=np.float32)
    raw = np.exp(-math.pi * offsets * offsets / (2.0 * LS * LS)).astype(np.float32)
    return (raw / np.sqrt(np.sum(raw * raw))).astype(ml_dtypes.bfloat16)


def pick(taps, index):
    inside = (index >= 0) & (index < TAPS)
    return np.where(inside, taps.astype(np.float32)[np.clip(index, 0, TAPS - 1)], 0.0)


def filter_weights(planes, rows):
    taps = filter_taps()
    span = pick(taps, np.arange(256)[None, :] - np.arange(128)[:, None] - 64 + FW)
    row = np.arange(rows)
    one = pick(taps, row[:, None] - row[None, :] + FW)
    quad = np.zeros((4 * rows, 4 * rows), np.float32)
    for q in range(4):
        quad[q * rows : (q + 1) * rows, q * rows : (q + 1) * rows] = one
    outer = np.concatenate([np.arange(FW) - FW, rows + np.arange(FW)])
    edge = pick(taps, outer[:, None] - row[None, :] + FW)
    halo = np.zeros((planes // 4, planes * 2 * FW, 4 * rows), np.float32)
    for m in range(planes):
        j, q = divmod(m, 4)
        halo[j, m * 2 * FW : (m + 1) * 2 * FW, q * rows : (q + 1) * rows] = edge
    cast = lambda a: jnp.asarray(a.astype(ml_dtypes.bfloat16))
    return cast(span), cast(quad), cast(halo)


def filter_kernel(left_ref, right_ref, hleft_ref, hright_ref, span_ref, quad_ref, halo_ref, out_ref):
    w = pl.program_id(0)
    planes, rows, lanes = left_ref.shape
    blocks = out_ref.shape[0]
    turned = (((1,), (1,)), ((), ()))
    window = jnp.concatenate([left_ref[...], right_ref[...]], axis=-1).reshape(planes * rows, 2 * lanes)
    edges = jnp.concatenate([hleft_ref[...], hright_ref[...]], axis=-1)
    band = span_ref[...]
    main = lax.dot_general(band, window, turned, preferred_element_type=F32).astype(BF16)
    edge = lax.dot_general(band, edges, turned, preferred_element_type=F32).astype(BF16)
    for j in range(planes // 4):
        part = jnp.dot(main[:, 4 * rows * j : 4 * rows * (j + 1)], quad_ref[...], preferred_element_type=F32)
        part += jnp.dot(edge, halo_ref[j], preferred_element_type=F32)
        part = part.astype(BF16)
        for h in range(2):
            t = lax.rem(2 * w + 1 + h, blocks)
            for k in range(2):
                out_ref[t, 2 * j + k] = part[64 * h : 64 * (h + 1), 128 * k : 128 * (k + 1)]


def filter_planes(noise, halo, weights):
    planes, rows, length = noise.shape
    windows = length // 128
    span, quad, edge = weights
    whole = lambda a: pl.BlockSpec(a.shape, lambda w: (0,) * a.ndim)
    return pl.pallas_call(
        filter_kernel,
        grid=(windows,),
        in_specs=[
            pl.BlockSpec((planes, rows, 128), lambda w: (0, 0, w)),
            pl.BlockSpec((planes, rows, 128), lambda w: (0, 0, lax.rem(w + 1, windows))),
            pl.BlockSpec((halo.shape[0], 128), lambda w: (0, w)),
            pl.BlockSpec((halo.shape[0], 128), lambda w: (0, lax.rem(w + 1, windows))),
            whole(span),
            whole(quad),
            whole(edge),
        ],
        out_specs=pl.BlockSpec((2 * windows, planes // 2, 64, 2 * rows), lambda w: (0, 0, 0, 0)),
        out_shape=jax.ShapeDtypeStruct((2 * windows, planes // 2, 64, 2 * rows), BF16),
        compiler_params=pltpu.CompilerParams(vmem_limit_bytes=40 * 2**20),
        name="filter",
    )(noise, noise, halo, halo, span, quad, edge)


def chain_kernel(
    got_ref, stress_ref, timescale_ref, mean_ref, courant_ref, prior_ref, field_ref, inflow_ref, result_ref, vel_ref
):
    groups, bands = got_ref.shape[:2]
    pairs = got_ref.shape[3]
    depth = got_ref.shape[4]
    per = 2 * pairs // 3
    steps = groups * per
    low = lax.broadcasted_iota(jnp.int32, (depth, 128), 1) < 64

    def band(b, _):
        lanes = pl.ds(pl.multiple_of(b * 128, 128), 128)
        courant = courant_ref[:, lanes]
        rest = 1.0 - courant
        inverse = 1.0 / rest
        decay = jnp.exp(-math.pi / (2.0 * timescale_ref[:, lanes]))
        gain = jnp.sqrt(1.0 - decay * decay)
        first = jnp.sqrt(stress_ref[0, :, lanes])
        second_low = stress_ref[1, :, lanes] / first
        second = jnp.sqrt(stress_ref[2, :, lanes] - second_low * second_low)
        third_low = stress_ref[3, :, lanes] / first
        third_mid = (stress_ref[4, :, lanes] - second_low * third_low) / second
        third = jnp.sqrt(stress_ref[5, :, lanes] - third_low * third_low - third_mid * third_mid)
        first, second_low, second = first * gain, second_low * gain, second * gain
        third_low, third_mid, third = third_low * gain, third_mid * gain, third * gain
        mean = mean_ref[:, lanes]
        phi = [prior_ref[m, :, lanes] / gain for m in range(3)]
        scale = courant * inverse
        for g in range(groups):
            planes = []
            for k in range(pairs):
                one = got_ref[g, b, 0, k].astype(F32)
                two = got_ref[g, b, 1, k].astype(F32)
                planes.append(jnp.where(low, one, pltpu.roll(two, 64, 1)))
                planes.append(jnp.where(low, pltpu.roll(one, 64, 1), two))
            for i in range(per):
                p = g * per + i
                phi = [decay * phi[m] + planes[3 * i + m] for m in range(3)]
                vel = (
                    mean + first * phi[0],
                    second_low * phi[0] + second * phi[1],
                    third_low * phi[0] + third_mid * phi[1] + third * phi[2],
                )
                for m in range(3):
                    inflow_ref[p, m, :, lanes] = vel[m].astype(BF16)
                    vel_ref[p, m] = vel[m] * scale
                scale = scale * inverse
        ratio = courant * inverse
        back = rest / courant
        square = rest * rest
        square = square * square
        square = square * square
        last = square * square
        for m in range(3):
            power = None
            cells = []
            for x in range(CX):
                start = field_ref[m, x, :, lanes]
                cells.append(start if x == 0 else start * power)
                power = back if x == 0 else power * back
            for p in range(steps):
                inlet = vel_ref[p, m]
                cells = [cells[x] + (inlet if x == 0 else cells[x - 1]) for x in range(CX)]
            power = last
            for x in range(CX):
                result_ref[m, x, :, lanes] = cells[x] * power
                power = power * ratio
        return _

    lax.fori_loop(0, bands, band, 0)


def march_cells(got, stress, timescale, mean, courant, prior, field):
    groups, bands, cores, pairs, depth, wide = got.shape
    rows = 16
    length = timescale.shape[1]
    steps = groups * 2 * pairs // 3
    spec = lambda *lead: pl.BlockSpec(lead + (rows, length), lambda s: (0,) * len(lead) + (s, 0))
    return pl.pallas_call(
        chain_kernel,
        grid=(depth // rows,),
        in_specs=[
            pl.BlockSpec((groups, bands, cores, pairs, rows, wide), lambda s: (0, 0, 0, 0, s, 0)),
            spec(6),
            spec(),
            spec(),
            spec(),
            spec(3),
            spec(3, CX),
        ],
        out_specs=[spec(steps, 3), spec(3, CX)],
        out_shape=[
            jax.ShapeDtypeStruct((steps, 3, depth, length), BF16),
            jax.ShapeDtypeStruct((3, CX, depth, length), F32),
        ],
        scratch_shapes=[pltpu.VMEM((steps, 3, rows, 128), F32)],
        compiler_params=pltpu.CompilerParams(vmem_limit_bytes=40 * 2**20),
        name="march",
    )(got, stress, timescale, mean, courant, prior, field)


def body(noise, stress, timescale, mean_inflow, courant, prior_state, field):
    per, comps, rows, length = noise.shape
    planes = per * comps
    tiles, groups = lax.axis_size("tile"), lax.axis_size("grp")
    noise = noise.reshape(planes, rows, length)
    up = [(i, i + 1) for i in range(tiles - 1)]
    down = [(i + 1, i) for i in range(tiles - 1)]
    before = lax.ppermute(noise[:, rows - FW :], "tile", up)
    after = lax.ppermute(noise[:, :FW], "tile", down)
    halo = jnp.concatenate([before, after], axis=1).reshape(planes * 2 * FW, length)
    blocks = filter_planes(noise, halo, filter_weights(planes, rows))
    got = lax.all_to_all(blocks, "tile", split_axis=0, concat_axis=0, tiled=True)
    got = got.reshape((groups, tiles // groups) + blocks.shape[1:])
    got = lax.all_to_all(got, "grp", split_axis=0, concat_axis=0, tiled=True)
    got = got.reshape((groups, tiles // groups // 2, 2) + blocks.shape[1:])
    inflow, result = march_cells(got, stress, timescale, mean_inflow, courant, prior_state, field)
    return (inflow, result)


def solution(mesh):
    placed = (
        P("grp", None, "tile", None),
        P(None, "tile", "grp"),
        P("tile", "grp"),
        P("tile", "grp"),
        P("tile", "grp"),
        P(None, "tile", "grp"),
        P(None, None, "tile", "grp"),
    )
    return jax.shard_map(
        body,
        mesh=mesh,
        in_specs=placed,
        out_specs=(P(None, None, "tile", "grp"), P(None, None, "tile", "grp")),
        check_vma=False,
    )
```

```python
import math

import jax
import jax.numpy as jnp
import ml_dtypes
import numpy as np
from jax import lax
from jax.experimental import pallas as pl
from jax.experimental.pallas import tpu as pltpu
from jax.sharding import PartitionSpec as P

LS = 2
FW = 4
TAPS = 2 * FW + 1
CX = 8
BF16 = jnp.bfloat16
F32 = jnp.float32
SIDE = 4
AXES = ("grp", "tile")


def filter_taps():
    offsets = np.arange(-FW, FW + 1, dtype=np.float32)
    raw = np.exp(-math.pi * offsets * offsets / (2.0 * LS * LS)).astype(np.float32)
    return (raw / np.sqrt(np.sum(raw * raw))).astype(ml_dtypes.bfloat16)


def pick(taps, index):
    inside = (index >= 0) & (index < TAPS)
    return np.where(inside, taps.astype(np.float32)[np.clip(index, 0, TAPS - 1)], 0.0)


def filter_weights(per, comps, rows):
    taps = filter_taps()
    span = pick(taps, np.arange(256)[None, :] - np.arange(128)[:, None] - 64 + FW)
    row = np.arange(rows)
    inner = pick(taps, row[:, None] - row[None, :] + FW)
    outer = np.concatenate([np.arange(FW) - FW, rows + np.arange(FW)])
    edge = pick(taps, outer[:, None] - row[None, :] + FW)
    wide = 2 * FW
    own = np.zeros((2, comps * rows, 4 * rows), np.float32)
    halo = np.zeros((per, per * comps * wide, 4 * rows), np.float32)
    for i in range(per):
        for m in range(comps):
            q = m if m < 2 else 2 + i % 2
            own[i % 2, m * rows : (m + 1) * rows, q * rows : (q + 1) * rows] = inner
            top = (i * comps + m) * wide
            halo[i, top : top + wide, q * rows : (q + 1) * rows] = edge
    cast = lambda a: jnp.asarray(a.astype(ml_dtypes.bfloat16))
    return cast(span), cast(own), cast(halo)


TURNED = (((1,), (1,)), ((), ()))


def whole(shape):
    return pl.BlockSpec(shape, lambda *_: (0,) * len(shape))


def cost(flops, traffic):
    return pl.CostEstimate(flops=flops, bytes_accessed=traffic, transcendentals=0)


VMEM = pl.BlockSpec(memory_space=pltpu.VMEM)


def span_kernel(noise_ref, band_ref, out_ref):
    i = pl.program_id(0)
    windows = noise_ref.shape[2] // 128
    for w in range(windows):
        if w < windows - 1:
            window = noise_ref[0, :, 128 * w : 128 * w + 256]
        else:
            window = jnp.concatenate([noise_ref[0, :, 128 * w :], noise_ref[0, :, :128]], axis=-1)
        out_ref[i, 128 * w : 128 * w + 128] = lax.dot_general(
            band_ref[...], window, TURNED, preferred_element_type=F32
        ).astype(BF16)


def span_planes(noise, band):
    per, rows, length = noise.shape
    return pl.pallas_call(
        span_kernel,
        grid=(per,),
        in_specs=[pl.BlockSpec((1, rows, length), lambda i: (i, 0, 0)), VMEM],
        out_specs=VMEM,
        out_shape=jax.ShapeDtypeStruct((per, length, rows), BF16),
        compiler_params=pltpu.CompilerParams(vmem_limit_bytes=12 * 2**20),
        cost_estimate=cost(2 * 10**9, 4 * 10**6),
        name="span",
    )(noise, band)


ROUNDS = [(r, (r + d) % SIDE) for d in range(SIDE) for r in range(SIDE)]


def seat():
    tile = lax.axis_index("tile")
    return lax.div(tile, 2 * SIDE), lax.rem(lax.div(tile, 2), SIDE), lax.rem(tile, 2), lax.axis_index("grp")


def rows_kernel(spans_ref, edges_ref, band_ref, own_ref, halo_ref, *refs):
    out_refs, done_ref = refs[:-1], refs[-1]
    per, length = spans_ref.shape[:2]
    windows, steps = 4, length // 512
    blocks = 2 * windows * steps
    band = band_ref[...]
    for step in range(steps):
        lo, hi = 512 * step, 512 * step + 640
        edges = edges_ref[:, lo:hi]
        if step == steps - 1:
            edges = jnp.concatenate([edges_ref[:, lo:], edges_ref[:, :128]], axis=-1)
        edge = jnp.concatenate(
            [
                lax.dot_general(
                    band, edges[:, 128 * v : 128 * v + 256], TURNED, preferred_element_type=F32
                ).astype(BF16)
                for v in range(windows)
            ],
            axis=0,
        )
        parts = [
            jnp.dot(spans_ref[i, lo : lo + 512], own_ref[i % 2], preferred_element_type=F32)
            + jnp.dot(edge, halo_ref[i], preferred_element_type=F32)
            for i in range(per)
        ]
        pairs = [part[:, :128] for part in parts]
        pairs += [parts[i][:, 128:] + parts[i + 1][:, 128:] for i in range(0, per, 2)]
        for k, pair in enumerate(pairs):
            pair = pair.astype(BF16)
            for v in range(2 * windows):
                done_ref[(2 * windows * step + 1 + v) % blocks, k] = pair[64 * v : 64 * (v + 1)]
    x, y, core, z = seat()
    for n, (r, d) in enumerate(ROUNDS):
        column = lax.rem(x - z + r + 2 * core + SIDE, SIDE)
        for h in range(2):
            target = (column * SIDE + lax.bitwise_xor(y, d)) * 2 + lax.rem(core + h, 2)
            out_refs[n][h] = done_ref[target]


def filter_rows(spans, halo, weights):
    block = (6, 64, 128)
    shapes = [(2,) + block] * len(ROUNDS)
    return pl.pallas_call(
        rows_kernel,
        in_specs=[VMEM] * 5,
        out_specs=[VMEM] * len(shapes),
        out_shape=[jax.ShapeDtypeStruct(a, BF16) for a in shapes],
        scratch_shapes=[pltpu.VMEM((4 * SIDE * 2,) + block, BF16)],
        compiler_params=pltpu.CompilerParams(vmem_limit_bytes=20 * 2**20),
        cost_estimate=cost(10**9, 4 * 10**6),
        name="rows",
    )(spans, halo, *weights)


def chain_kernel(*refs):
    count = len(ROUNDS)
    stay_refs, swap_refs = refs[:count], refs[count : count + 2]
    stress_ref, timescale_ref, mean_ref, courant_ref, prior_ref, field_ref = refs[count + 2 : count + 8]
    inflow_ref, result_ref, vel_ref, held_ref = refs[count + 8 :]
    groups, per = SIDE, 4
    depth = timescale_ref.shape[0]
    steps = groups * per
    low = lax.broadcasted_iota(jnp.int32, (depth, 128), 1) < 64
    x, y, core, z = seat()
    for n, (r, d) in enumerate(ROUNDS):
        for h in range(2):
            came = lax.rem(core + h, 2)
            time = lax.rem(z - x + r + 2 * came + SIDE, SIDE)
            half, place_in = divmod(n, count // 2)
            held_ref[came, time, d] = stay_refs[n][0] if h == 0 else swap_refs[half][place_in]

    def band(d, _):
        lanes = pl.ds(pl.multiple_of(lax.bitwise_xor(y, d) * 128, 128), 128)
        courant = courant_ref[:, lanes]
        rest = 1.0 - courant
        inverse = 1.0 / rest
        decay = jnp.exp(-math.pi / (2.0 * timescale_ref[:, lanes]))
        gain = jnp.sqrt(1.0 - decay * decay)
        first = jnp.sqrt(stress_ref[0, :, lanes])
        second_low = stress_ref[1, :, lanes] / first
        second = jnp.sqrt(stress_ref[2, :, lanes] - second_low * second_low)
        third_low = stress_ref[3, :, lanes] / first
        third_mid = (stress_ref[4, :, lanes] - second_low * third_low) / second
        third = jnp.sqrt(stress_ref[5, :, lanes] - third_low * third_low - third_mid * third_mid)
        first, second_low, second = first * gain, second_low * gain, second * gain
        third_low, third_mid, third = third_low * gain, third_mid * gain, third * gain
        mean = mean_ref[:, lanes]
        phi = [prior_ref[m, :, lanes] / gain for m in range(3)]
        ratio = courant * inverse
        scale = ratio
        for g in range(groups):

            def pair(k):
                one, two = [held_ref[came, g, d, k].astype(F32) for came in range(2)]
                return jnp.where(low, one, pltpu.roll(two, 64, 1)), jnp.where(low, pltpu.roll(one, 64, 1), two)

            for half in range(2):
                third_planes = pair(4 + half)
                for i in range(2):
                    p = g * per + 2 * half + i
                    planes = (*pair(2 * half + i), third_planes[i])
                    phi = [decay * phi[m] + planes[m] for m in range(3)]
                    vel = (
                        mean + first * phi[0],
                        second_low * phi[0] + second * phi[1],
                        third_low * phi[0] + third_mid * phi[1] + third * phi[2],
                    )
                    for m in range(3):
                        inflow_ref[p, m, :, lanes] = vel[m].astype(BF16)
                        vel_ref[p, m] = vel[m] * scale
                    scale = scale * inverse
        back = rest / courant
        square = rest * rest
        square = square * square
        square = square * square
        last = square * square
        for m in range(3):
            power = None
            cells = []
            for j in range(CX):
                start = field_ref[m, j, :, lanes]
                cells.append(start if j == 0 else start * power)
                power = back if j == 0 else power * back
            for p in range(steps):
                inlet = vel_ref[p, m]
                cells = [cells[j] + (inlet if j == 0 else cells[j - 1]) for j in range(CX)]
            power = last
            for j in range(CX):
                result_ref[m, j, :, lanes] = cells[j] * power
                power = power * ratio
        return _

    lax.fori_loop(0, SIDE, band, 0)


def march_cells(stay, swap, stress, timescale, mean, courant, prior, field):
    rows = 16
    depth, length = timescale.shape
    steps = 16
    spec = lambda *lead: pl.BlockSpec(lead + (rows, length), lambda s: (0,) * len(lead) + (s, 0))
    return pl.pallas_call(
        chain_kernel,
        grid=(depth // rows,),
        in_specs=[pl.BlockSpec((1, 6, rows, 128), lambda s: (0, 0, s, 0))] * len(stay)
        + [pl.BlockSpec((len(stay) // 2, 6, rows, 128), lambda s: (0, 0, s, 0))] * 2
        + [spec(6), spec(), spec(), spec(), spec(3), spec(3, CX)],
        out_specs=[spec(steps, 3), spec(3, CX)],
        out_shape=[
            jax.ShapeDtypeStruct((steps, 3, depth, length), BF16),
            jax.ShapeDtypeStruct((3, CX, depth, length), F32),
        ],
        scratch_shapes=[
            pltpu.VMEM((steps, 3, rows, 128), F32),
            pltpu.VMEM((2, SIDE, SIDE, 6, rows, 128), BF16),
        ],
        compiler_params=pltpu.CompilerParams(vmem_limit_bytes=32 * 2**20),
        cost_estimate=cost(10**9, 14 * 10**6),
        name="march",
    )(*stay, *swap, stress, timescale, mean, courant, prior, field)


def place(x, y, core, z):
    return z * 32 + (x * SIDE + y) * 2 + core


def moves(target):
    seats = [(x, y, core, z) for x in range(SIDE) for y in range(SIDE) for core in range(2) for z in range(SIDE)]
    return [(place(*one), place(*target(*one))) for one in seats]


def exchange(blocks):
    got = []
    for block, (r, d) in zip(blocks, ROUNDS, strict=True):
        pairs = moves(lambda x, y, core, z: ((x - z + r + 2 * core) % SIDE, y ^ d, core, x))
        got.append(lax.ppermute(block, AXES, pairs))
    return got


def body(noise, stress, timescale, mean_inflow, courant, prior_state, field):
    per, comps, rows, length = noise.shape
    tiles = lax.axis_size("tile")
    flat = noise.reshape(per * comps, rows, length)
    up = [(i, i + 1) for i in range(tiles - 1)]
    down = [(i + 1, i) for i in range(tiles - 1)]
    before = lax.ppermute(flat[:, rows - FW :], "tile", up)
    after = lax.ppermute(flat[:, :FW], "tile", down)
    halo = jnp.concatenate([before, after], axis=1).reshape(per * comps * 2 * FW, length)
    weights = filter_weights(per, comps, rows)
    spans = span_planes(noise.reshape(per, comps * rows, length), weights[0])
    got = exchange(filter_rows(spans, halo, weights))
    other = moves(lambda x, y, core, z: (x, y, 1 - core, z))
    half = len(got) // 2
    swap = [lax.ppermute(jnp.stack([a[1] for a in part]), AXES, other) for part in (got[:half], got[half:])]
    inflow, result = march_cells(got, swap, stress, timescale, mean_inflow, courant, prior_state, field)
    return (inflow, result)


def solution(mesh):
    placed = (
        P("grp", None, "tile", None),
        P(None, "tile", "grp"),
        P("tile", "grp"),
        P("tile", "grp"),
        P("tile", "grp"),
        P(None, "tile", "grp"),
        P(None, None, "tile", "grp"),
    )
    return jax.shard_map(
        body,
        mesh=mesh,
        in_specs=placed,
        out_specs=(P(None, None, "tile", "grp"), P(None, None, "tile", "grp")),
        check_vma=False,
    )
```

```python
import math

import jax
import jax.numpy as jnp
import ml_dtypes
import numpy as np
from jax import lax
from jax.experimental import pallas as pl
from jax.experimental.pallas import tpu as pltpu
from jax.sharding import PartitionSpec as P


LS = 2
FW = 4
TAPS = 2 * FW + 1
CX = 8
BF16 = jnp.bfloat16
F32 = jnp.float32
SIDE = 4
AXES = ("grp", "tile")


def filter_taps():
    offsets = np.arange(-FW, FW + 1, dtype=np.float32)
    raw = np.exp(-math.pi * offsets * offsets / (2.0 * LS * LS)).astype(np.float32)
    return (raw / np.sqrt(np.sum(raw * raw))).astype(ml_dtypes.bfloat16)


def pick(taps, index):
    inside = (index >= 0) & (index < TAPS)
    return np.where(inside, taps.astype(np.float32)[np.clip(index, 0, TAPS - 1)], 0.0)


def filter_weights(per, comps, rows):
    taps = filter_taps()
    span = pick(taps, np.arange(256)[None, :] - np.arange(128)[:, None] - 64 + FW)
    row = np.arange(rows)
    inner = pick(taps, row[:, None] - row[None, :] + FW)
    outer = np.concatenate([np.arange(FW) - FW, rows + np.arange(FW)])
    edge = pick(taps, outer[:, None] - row[None, :] + FW)
    wide = 2 * FW
    own = np.zeros((2, comps * rows, 4 * rows), np.float32)
    halo = np.zeros((per, per * comps * wide, 4 * rows), np.float32)
    for i in range(per):
        for m in range(comps):
            q = m if m < 2 else 2 + i % 2
            own[i % 2, m * rows : (m + 1) * rows, q * rows : (q + 1) * rows] = inner
            top = (i * comps + m) * wide
            halo[i, top : top + wide, q * rows : (q + 1) * rows] = edge
    cast = lambda a: jnp.asarray(a.astype(ml_dtypes.bfloat16))
    return cast(span), cast(own), cast(halo)


TURNED = (((1,), (1,)), ((), ()))


def cost(flops, traffic):
    return pl.CostEstimate(flops=flops, bytes_accessed=traffic, transcendentals=0)


VMEM = pl.BlockSpec(memory_space=pltpu.VMEM)


def span_kernel(noise_ref, band_ref, out_ref):
    i = pl.program_id(0)
    windows = noise_ref.shape[2] // 128
    for w in range(windows):
        if w < windows - 1:
            window = noise_ref[0, :, 128 * w : 128 * w + 256]
        else:
            window = jnp.concatenate([noise_ref[0, :, 128 * w :], noise_ref[0, :, :128]], axis=-1)
        out_ref[i, 128 * w : 128 * w + 128] = lax.dot_general(
            band_ref[...], window, TURNED, preferred_element_type=F32
        ).astype(BF16)


def span_planes(noise, band):
    per, rows, length = noise.shape
    return pl.pallas_call(
        span_kernel,
        grid=(per,),
        in_specs=[pl.BlockSpec((1, rows, length), lambda i: (i, 0, 0)), VMEM],
        out_specs=VMEM,
        out_shape=jax.ShapeDtypeStruct((per, length, rows), BF16),
        compiler_params=pltpu.CompilerParams(vmem_limit_bytes=12 * 2**20),
        cost_estimate=cost(2 * 10**9, 4 * 10**6),
        name="span",
    )(noise, band)


ROUNDS = [(r, (d - r) % SIDE) for d in range(SIDE) for r in range(SIDE)]
SOON = 12


def seat():
    tile = lax.axis_index("tile")
    return lax.div(tile, 2 * SIDE), lax.rem(lax.div(tile, 2), SIDE), lax.rem(tile, 2), lax.axis_index("grp")


def rows_kernel(spans_ref, edges_ref, band_ref, own_ref, halo_ref, *refs):
    out_refs, done_ref = refs[:-1], refs[-1]
    per, length = spans_ref.shape[:2]
    windows, steps = 4, length // 512
    blocks = 2 * windows * steps
    band = band_ref[...]
    for step in range(steps):
        lo, hi = 512 * step, 512 * step + 640
        edges = edges_ref[:, lo:hi]
        if step == steps - 1:
            edges = jnp.concatenate([edges_ref[:, lo:], edges_ref[:, :128]], axis=-1)
        edge = jnp.concatenate(
            [
                lax.dot_general(
                    band, edges[:, 128 * v : 128 * v + 256], TURNED, preferred_element_type=F32
                ).astype(BF16)
                for v in range(windows)
            ],
            axis=0,
        )
        parts = [
            jnp.dot(spans_ref[i, lo : lo + 512], own_ref[i % 2], preferred_element_type=F32)
            + jnp.dot(edge, halo_ref[i], preferred_element_type=F32)
            for i in range(per)
        ]
        pairs = [part[:, :128] for part in parts]
        pairs += [parts[i][:, 128:] + parts[i + 1][:, 128:] for i in range(0, per, 2)]
        for k, pair in enumerate(pairs):
            pair = pair.astype(BF16)
            for v in range(2 * windows):
                done_ref[(2 * windows * step + 1 + v) % blocks, k] = pair[64 * v : 64 * (v + 1)]
    x, y, core, z = seat()
    for n, (r, d) in enumerate(ROUNDS):
        column = lax.rem(x - z + r + 2 * core + SIDE, SIDE)
        for h in range(2):
            target = (column * SIDE + lax.bitwise_xor(y, d)) * 2 + lax.rem(core + h, 2)
            out_refs[n][h] = done_ref[target]


def filter_rows(spans, halo, weights):
    block = (6, 64, 128)
    shapes = [(2,) + block] * len(ROUNDS)
    return pl.pallas_call(
        rows_kernel,
        in_specs=[VMEM] * 5,
        out_specs=[VMEM] * len(shapes),
        out_shape=[jax.ShapeDtypeStruct(a, BF16) for a in shapes],
        scratch_shapes=[pltpu.VMEM((4 * SIDE * 2,) + block, BF16)],
        compiler_params=pltpu.CompilerParams(vmem_limit_bytes=20 * 2**20),
        cost_estimate=cost(10**9, 4 * 10**6),
        name="rows",
    )(spans, halo, *weights)


def chain_kernel(*refs):
    count = len(ROUNDS)
    stay_refs, swap_refs = refs[:count], refs[count : count + 2]
    stress_ref, timescale_ref, mean_ref, courant_ref, prior_ref, field_ref = refs[count + 2 : count + 8]
    inflow_ref, result_ref, vel_ref, held_ref = refs[count + 8 :]
    groups, per = SIDE, 4
    depth = timescale_ref.shape[0]
    steps = groups * per
    low = lax.broadcasted_iota(jnp.int32, (depth, 128), 1) < 64
    x, y, core, z = seat()
    for n, (r, d) in enumerate(ROUNDS):
        for h in range(2):
            came = lax.rem(core + h, 2)
            time = lax.rem(z - x + r + 2 * came + SIDE, SIDE)
            if h == 0:
                held_ref[came, time, d] = stay_refs[n][0]
            else:
                held_ref[came, time, d] = swap_refs[0][n] if n < SOON else swap_refs[1][n - SOON]

    def band(d, _):
        lanes = pl.ds(pl.multiple_of(lax.bitwise_xor(y, d) * 128, 128), 128)
        courant = courant_ref[:, lanes]
        rest = 1.0 - courant
        inverse = 1.0 / rest
        decay = jnp.exp(-math.pi / (2.0 * timescale_ref[:, lanes]))
        gain = jnp.sqrt(1.0 - decay * decay)
        first = jnp.sqrt(stress_ref[0, :, lanes])
        second_low = stress_ref[1, :, lanes] / first
        second = jnp.sqrt(stress_ref[2, :, lanes] - second_low * second_low)
        third_low = stress_ref[3, :, lanes] / first
        third_mid = (stress_ref[4, :, lanes] - second_low * third_low) / second
        third = jnp.sqrt(stress_ref[5, :, lanes] - third_low * third_low - third_mid * third_mid)
        first, second_low, second = first * gain, second_low * gain, second * gain
        third_low, third_mid, third = third_low * gain, third_mid * gain, third * gain
        mean = mean_ref[:, lanes]
        phi = [prior_ref[m, :, lanes] / gain for m in range(3)]
        ratio = courant * inverse
        scale = ratio
        for g in range(groups):

            def pair(k):
                one, two = [held_ref[came, g, d, k].astype(F32) for came in range(2)]
                return jnp.where(low, one, pltpu.roll(two, 64, 1)), jnp.where(low, pltpu.roll(one, 64, 1), two)

            for half in range(2):
                third_planes = pair(4 + half)
                for i in range(2):
                    p = g * per + 2 * half + i
                    planes = (*pair(2 * half + i), third_planes[i])
                    phi = [decay * phi[m] + planes[m] for m in range(3)]
                    vel = (
                        mean + first * phi[0],
                        second_low * phi[0] + second * phi[1],
                        third_low * phi[0] + third_mid * phi[1] + third * phi[2],
                    )
                    for m in range(3):
                        inflow_ref[p, m, :, lanes] = vel[m].astype(BF16)
                        vel_ref[p, m] = vel[m] * scale
                    scale = scale * inverse
        back = rest / courant
        square = rest * rest
        square = square * square
        square = square * square
        last = square * square
        for m in range(3):
            power = None
            cells = []
            for j in range(CX):
                start = field_ref[m, j, :, lanes]
                cells.append(start if j == 0 else start * power)
                power = back if j == 0 else power * back
            for p in range(steps):
                inlet = vel_ref[p, m]
                cells = [cells[j] + (inlet if j == 0 else cells[j - 1]) for j in range(CX)]
            power = last
            for j in range(CX):
                result_ref[m, j, :, lanes] = cells[j] * power
                power = power * ratio
        return _

    lax.fori_loop(0, SIDE, band, 0)


def march_cells(stay, swap, stress, timescale, mean, courant, prior, field):
    rows = 16
    depth, length = timescale.shape
    steps = 16
    spec = lambda *lead: pl.BlockSpec(lead + (rows, length), lambda s: (0,) * len(lead) + (s, 0))
    return pl.pallas_call(
        chain_kernel,
        grid=(depth // rows,),
        in_specs=[pl.BlockSpec((1, 6, rows, 128), lambda s: (0, 0, s, 0))] * len(stay)
        + [pl.BlockSpec((part.shape[0], 6, rows, 128), lambda s: (0, 0, s, 0)) for part in swap]
        + [spec(6), spec(), spec(), spec(), spec(3), spec(3, CX)],
        out_specs=[spec(steps, 3), spec(3, CX)],
        out_shape=[
            jax.ShapeDtypeStruct((steps, 3, depth, length), BF16),
            jax.ShapeDtypeStruct((3, CX, depth, length), F32),
        ],
        scratch_shapes=[
            pltpu.VMEM((steps, 3, rows, 128), F32),
            pltpu.VMEM((2, SIDE, SIDE, 6, rows, 128), BF16),
        ],
        compiler_params=pltpu.CompilerParams(vmem_limit_bytes=32 * 2**20),
        cost_estimate=cost(10**9, 14 * 10**6),
        name="march",
    )(*stay, *swap, stress, timescale, mean, courant, prior, field)


def place(x, y, core, z):
    return z * 32 + (x * SIDE + y) * 2 + core


def moves(target):
    seats = [(x, y, core, z) for x in range(SIDE) for y in range(SIDE) for core in range(2) for z in range(SIDE)]
    return [(place(*one), place(*target(*one))) for one in seats]


def exchange(blocks):
    got = []
    for block, (r, d) in zip(blocks, ROUNDS, strict=True):
        pairs = moves(lambda x, y, core, z: ((x - z + r + 2 * core) % SIDE, y ^ d, core, x))
        got.append(lax.ppermute(block, AXES, pairs))
    return got


def body(noise, stress, timescale, mean_inflow, courant, prior_state, field):
    per, comps, rows, length = noise.shape
    tiles = lax.axis_size("tile")
    flat = noise.reshape(per * comps, rows, length)
    up = [(i, i + 1) for i in range(tiles - 1)]
    down = [(i + 1, i) for i in range(tiles - 1)]
    before = lax.ppermute(flat[:, rows - FW :], "tile", up)
    after = lax.ppermute(flat[:, :FW], "tile", down)
    halo = jnp.concatenate([before, after], axis=1).reshape(per * comps * 2 * FW, length)
    weights = filter_weights(per, comps, rows)
    spans = span_planes(noise.reshape(per, comps * rows, length), weights[0])
    other = moves(lambda x, y, core, z: (x, y, 1 - core, z))
    swap = []
    got = exchange(filter_rows(spans, halo, weights))
    for part in (got[:SOON], got[SOON:]):
        swap.append(lax.ppermute(jnp.stack([a[1] for a in part]), AXES, other))
    inflow, result = march_cells(got, swap, stress, timescale, mean_inflow, courant, prior_state, field)
    return (inflow, result)


def solution(mesh):
    placed = (
        P("grp", None, "tile", None),
        P(None, "tile", "grp"),
        P("tile", "grp"),
        P("tile", "grp"),
        P("tile", "grp"),
        P(None, "tile", "grp"),
        P(None, None, "tile", "grp"),
    )
    return jax.shard_map(
        body,
        mesh=mesh,
        in_specs=placed,
        out_specs=(P(None, None, "tile", "grp"), P(None, None, "tile", "grp")),
        check_vma=False,
    )
```

```python
import math

import jax
import jax.numpy as jnp
import ml_dtypes
import numpy as np
from jax import lax
from jax.experimental import pallas as pl
from jax.experimental.pallas import tpu as pltpu
from jax.sharding import PartitionSpec as P


LS = 2
FW = 4
TAPS = 2 * FW + 1
CX = 8
BF16 = jnp.bfloat16
F32 = jnp.float32
SIDE = 4
AXES = ("grp", "tile")


def filter_taps():
    offsets = np.arange(-FW, FW + 1, dtype=np.float32)
    raw = np.exp(-math.pi * offsets * offsets / (2.0 * LS * LS)).astype(np.float32)
    return (raw / np.sqrt(np.sum(raw * raw))).astype(ml_dtypes.bfloat16)


def pick(taps, index):
    inside = (index >= 0) & (index < TAPS)
    return np.where(inside, taps.astype(np.float32)[np.clip(index, 0, TAPS - 1)], 0.0)


def filter_weights(per, comps, rows):
    taps = filter_taps()
    span = pick(taps, np.arange(256)[None, :] - np.arange(128)[:, None] - 64 + FW)
    row = np.arange(rows)
    inner = pick(taps, row[:, None] - row[None, :] + FW)
    outer = np.concatenate([np.arange(FW) - FW, rows + np.arange(FW)])
    edge = pick(taps, outer[:, None] - row[None, :] + FW)
    wide = 2 * FW
    own = np.zeros((2, comps * rows, 4 * rows), np.float32)
    halo = np.zeros((per, per * comps * wide, 4 * rows), np.float32)
    for i in range(per):
        for m in range(comps):
            q = m if m < 2 else 2 + i % 2
            own[i % 2, m * rows : (m + 1) * rows, q * rows : (q + 1) * rows] = inner
            top = (i * comps + m) * wide
            halo[i, top : top + wide, q * rows : (q + 1) * rows] = edge
    cast = lambda a: jnp.asarray(a.astype(ml_dtypes.bfloat16))
    return cast(span), cast(own), cast(halo)


TURNED = (((1,), (1,)), ((), ()))


def cost(flops, traffic):
    return pl.CostEstimate(flops=flops, bytes_accessed=traffic, transcendentals=0)


VMEM = pl.BlockSpec(memory_space=pltpu.VMEM)


def span_kernel(noise_ref, band_ref, out_ref):
    i = pl.program_id(0)
    windows = noise_ref.shape[2] // 128
    for w in range(windows):
        if w < windows - 1:
            window = noise_ref[0, :, 128 * w : 128 * w + 256]
        else:
            window = jnp.concatenate([noise_ref[0, :, 128 * w :], noise_ref[0, :, :128]], axis=-1)
        out_ref[i, 128 * w : 128 * w + 128] = lax.dot_general(
            band_ref[...], window, TURNED, preferred_element_type=F32
        ).astype(BF16)


def span_planes(noise, band):
    per, rows, length = noise.shape
    return pl.pallas_call(
        span_kernel,
        grid=(per,),
        in_specs=[pl.BlockSpec((1, rows, length), lambda i: (i, 0, 0)), VMEM],
        out_specs=VMEM,
        out_shape=jax.ShapeDtypeStruct((per, length, rows), BF16),
        compiler_params=pltpu.CompilerParams(vmem_limit_bytes=12 * 2**20),
        cost_estimate=cost(2 * 10**9, 4 * 10**6),
        name="span",
    )(noise, band)


ROUNDS = [(r, (d - r) % SIDE) for d in range(SIDE) for r in range(SIDE)]
SOON = 12


def seat():
    tile = lax.axis_index("tile")
    return lax.div(tile, 2 * SIDE), lax.rem(lax.div(tile, 2), SIDE), lax.rem(tile, 2), lax.axis_index("grp")


def rows_kernel(spans_ref, edges_ref, band_ref, own_ref, halo_ref, *refs):
    out_refs, done_ref = refs[:-1], refs[-1]
    per, length = spans_ref.shape[:2]
    windows, steps = 4, length // 512
    blocks = 2 * windows * steps
    band = band_ref[...]
    for step in range(steps):
        lo, hi = 512 * step, 512 * step + 640
        edges = edges_ref[:, lo:hi]
        if step == steps - 1:
            edges = jnp.concatenate([edges_ref[:, lo:], edges_ref[:, :128]], axis=-1)
        edge = jnp.concatenate(
            [
                lax.dot_general(
                    band, edges[:, 128 * v : 128 * v + 256], TURNED, preferred_element_type=F32
                ).astype(BF16)
                for v in range(windows)
            ],
            axis=0,
        )
        parts = [
            jnp.dot(spans_ref[i, lo : lo + 512], own_ref[i % 2], preferred_element_type=F32)
            + jnp.dot(edge, halo_ref[i], preferred_element_type=F32)
            for i in range(per)
        ]
        pairs = [part[:, :128] for part in parts]
        pairs += [parts[i][:, 128:] + parts[i + 1][:, 128:] for i in range(0, per, 2)]
        for k, pair in enumerate(pairs):
            pair = pair.astype(BF16)
            for v in range(2 * windows):
                done_ref[(2 * windows * step + 1 + v) % blocks, k] = pair[64 * v : 64 * (v + 1)]
    x, y, core, z = seat()
    for n, (r, d) in enumerate(ROUNDS):
        column = lax.rem(x - z + r + 2 * core + SIDE, SIDE)
        for h in range(2):
            target = (column * SIDE + lax.bitwise_xor(y, d)) * 2 + lax.rem(core + h, 2)
            out_refs[n][h] = done_ref[target]


def filter_rows(spans, halo, weights):
    block = (6, 64, 128)
    shapes = [(2,) + block] * len(ROUNDS)
    return pl.pallas_call(
        rows_kernel,
        in_specs=[VMEM] * 5,
        out_specs=[VMEM] * len(shapes),
        out_shape=[jax.ShapeDtypeStruct(a, BF16) for a in shapes],
        scratch_shapes=[pltpu.VMEM((4 * SIDE * 2,) + block, BF16)],
        compiler_params=pltpu.CompilerParams(vmem_limit_bytes=20 * 2**20),
        cost_estimate=cost(10**9, 4 * 10**6),
        name="rows",
    )(spans, halo, *weights)


def chain_kernel(*refs):
    count = len(ROUNDS)
    stay_refs, swap_refs = refs[:count], refs[count : count + 2]
    stress_ref, timescale_ref, mean_ref, courant_ref, prior_ref, field_ref = refs[count + 2 : count + 8]
    inflow_ref, result_ref, vel_ref, held_ref = refs[count + 8 :]
    groups, per = SIDE, 4
    depth = timescale_ref.shape[0]
    steps = groups * per
    low = lax.broadcasted_iota(jnp.int32, (depth, 128), 1) < 64
    x, y, core, z = seat()
    rows = pl.ds(pl.multiple_of(pl.program_id(0) * depth, depth), depth)
    for n, (r, d) in enumerate(ROUNDS):
        for h in range(2):
            came = lax.rem(core + h, 2)
            time = lax.rem(z - x + r + 2 * came + SIDE, SIDE)
            if h == 0:
                held_ref[came, time, d] = stay_refs[n][0, :, rows]
            else:
                held_ref[came, time, d] = swap_refs[0][n, :, rows] if n < SOON else swap_refs[1][n - SOON, :, rows]

    def band(d, _):
        lanes = pl.ds(pl.multiple_of(lax.bitwise_xor(y, d) * 128, 128), 128)
        courant = courant_ref[:, lanes]
        rest = 1.0 - courant
        inverse = 1.0 / rest
        decay = jnp.exp(-math.pi / (2.0 * timescale_ref[:, lanes]))
        gain = jnp.sqrt(1.0 - decay * decay)
        first = jnp.sqrt(stress_ref[0, :, lanes])
        second_low = stress_ref[1, :, lanes] / first
        second = jnp.sqrt(stress_ref[2, :, lanes] - second_low * second_low)
        third_low = stress_ref[3, :, lanes] / first
        third_mid = (stress_ref[4, :, lanes] - second_low * third_low) / second
        third = jnp.sqrt(stress_ref[5, :, lanes] - third_low * third_low - third_mid * third_mid)
        first, second_low, second = first * gain, second_low * gain, second * gain
        third_low, third_mid, third = third_low * gain, third_mid * gain, third * gain
        mean = mean_ref[:, lanes]
        phi = [prior_ref[m, :, lanes] / gain for m in range(3)]
        ratio = courant * inverse
        scale = ratio
        for g in range(groups):

            def pair(k):
                one, two = [held_ref[came, g, d, k].astype(F32) for came in range(2)]
                return jnp.where(low, one, pltpu.roll(two, 64, 1)), jnp.where(low, pltpu.roll(one, 64, 1), two)

            for half in range(2):
                third_planes = pair(4 + half)
                for i in range(2):
                    p = g * per + 2 * half + i
                    planes = (*pair(2 * half + i), third_planes[i])
                    phi = [decay * phi[m] + planes[m] for m in range(3)]
                    vel = (
                        mean + first * phi[0],
                        second_low * phi[0] + second * phi[1],
                        third_low * phi[0] + third_mid * phi[1] + third * phi[2],
                    )
                    for m in range(3):
                        inflow_ref[p, m, :, lanes] = vel[m].astype(BF16)
                        vel_ref[p, m] = vel[m] * scale
                    scale = scale * inverse
        back = rest / courant
        square = rest * rest
        square = square * square
        square = square * square
        last = square * square
        for m in range(3):
            power = None
            cells = []
            for j in range(CX):
                start = field_ref[m, j, :, lanes]
                cells.append(start if j == 0 else start * power)
                power = back if j == 0 else power * back
            for p in range(steps):
                inlet = vel_ref[p, m]
                cells = [cells[j] + (inlet if j == 0 else cells[j - 1]) for j in range(CX)]
            power = last
            for j in range(CX):
                result_ref[m, j, :, lanes] = cells[j] * power
                power = power * ratio
        return _

    lax.fori_loop(0, SIDE, band, 0)


def march_cells(stay, swap, stress, timescale, mean, courant, prior, field):
    rows = 16
    depth, length = timescale.shape
    steps = 16
    spec = lambda *lead: pl.BlockSpec(lead + (rows, length), lambda s: (0,) * len(lead) + (s, 0))
    return pl.pallas_call(
        chain_kernel,
        grid=(depth // rows,),
        in_specs=[VMEM] * (len(stay) + len(swap))
        + [spec(6), spec(), spec(), spec(), spec(3), spec(3, CX)],
        out_specs=[spec(steps, 3), spec(3, CX)],
        out_shape=[
            jax.ShapeDtypeStruct((steps, 3, depth, length), BF16),
            jax.ShapeDtypeStruct((3, CX, depth, length), F32),
        ],
        scratch_shapes=[
            pltpu.VMEM((steps, 3, rows, 128), F32),
            pltpu.VMEM((2, SIDE, SIDE, 6, rows, 128), BF16),
        ],
        compiler_params=pltpu.CompilerParams(vmem_limit_bytes=32 * 2**20),
        cost_estimate=cost(10**9, 14 * 10**6),
        name="march",
    )(*stay, *swap, stress, timescale, mean, courant, prior, field)


def place(x, y, core, z):
    return z * 32 + (x * SIDE + y) * 2 + core


def moves(target):
    seats = [(x, y, core, z) for x in range(SIDE) for y in range(SIDE) for core in range(2) for z in range(SIDE)]
    return [(place(*one), place(*target(*one))) for one in seats]


def exchange(blocks):
    got = []
    for block, (r, d) in zip(blocks, ROUNDS, strict=True):
        pairs = moves(lambda x, y, core, z: ((x - z + r + 2 * core) % SIDE, y ^ d, core, x))
        got.append(lax.ppermute(block, AXES, pairs))
    return got


def body(noise, stress, timescale, mean_inflow, courant, prior_state, field):
    per, comps, rows, length = noise.shape
    tiles = lax.axis_size("tile")
    flat = noise.reshape(per * comps, rows, length)
    up = [(i, i + 1) for i in range(tiles - 1)]
    down = [(i + 1, i) for i in range(tiles - 1)]
    before = lax.ppermute(flat[:, rows - FW :], "tile", up)
    after = lax.ppermute(flat[:, :FW], "tile", down)
    halo = jnp.concatenate([before, after], axis=1).reshape(per * comps * 2 * FW, length)
    weights = filter_weights(per, comps, rows)
    spans = span_planes(noise.reshape(per, comps * rows, length), weights[0])
    other = moves(lambda x, y, core, z: (x, y, 1 - core, z))
    swap = []
    got = exchange(filter_rows(spans, halo, weights))
    for part in (got[:SOON], got[SOON:]):
        swap.append(lax.ppermute(jnp.stack([a[1] for a in part]), AXES, other))
    inflow, result = march_cells(got, swap, stress, timescale, mean_inflow, courant, prior_state, field)
    return (inflow, result)


def solution(mesh):
    placed = (
        P("grp", None, "tile", None),
        P(None, "tile", "grp"),
        P("tile", "grp"),
        P("tile", "grp"),
        P("tile", "grp"),
        P(None, "tile", "grp"),
        P(None, None, "tile", "grp"),
    )
    return jax.shard_map(
        body,
        mesh=mesh,
        in_specs=placed,
        out_specs=(P(None, None, "tile", "grp"), P(None, None, "tile", "grp")),
        check_vma=False,
    )
```

```python
import math

import jax
import jax.numpy as jnp
import ml_dtypes
import numpy as np
from jax import lax
from jax.experimental import pallas as pl
from jax.experimental.pallas import tpu as pltpu
from jax.sharding import PartitionSpec as P


LS = 2
FW = 4
TAPS = 2 * FW + 1
CX = 8
BF16 = jnp.bfloat16
F32 = jnp.float32
SIDE = 4
AXES = ("grp", "tile")


def filter_taps():
    offsets = np.arange(-FW, FW + 1, dtype=np.float32)
    raw = np.exp(-math.pi * offsets * offsets / (2.0 * LS * LS)).astype(np.float32)
    return (raw / np.sqrt(np.sum(raw * raw))).astype(ml_dtypes.bfloat16)


def pick(taps, index):
    inside = (index >= 0) & (index < TAPS)
    return np.where(inside, taps.astype(np.float32)[np.clip(index, 0, TAPS - 1)], 0.0)


def filter_weights(per, comps, rows):
    taps = filter_taps()
    span = pick(taps, np.arange(256)[None, :] - np.arange(128)[:, None] - 64 + FW)
    row = np.arange(rows)
    inner = pick(taps, row[:, None] - row[None, :] + FW)
    outer = np.concatenate([np.arange(FW) - FW, rows + np.arange(FW)])
    edge = pick(taps, outer[:, None] - row[None, :] + FW)
    wide = 2 * FW
    own = np.zeros((2, comps * rows, 4 * rows), np.float32)
    halo = np.zeros((per, per * comps * wide, 4 * rows), np.float32)
    for i in range(per):
        for m in range(comps):
            q = m if m < 2 else 2 + i % 2
            own[i % 2, m * rows : (m + 1) * rows, q * rows : (q + 1) * rows] = inner
            top = (i * comps + m) * wide
            halo[i, top : top + wide, q * rows : (q + 1) * rows] = edge
    cast = lambda a: jnp.asarray(a.astype(ml_dtypes.bfloat16))
    return cast(span), cast(own), cast(halo)


TURNED = (((1,), (1,)), ((), ()))


def cost(flops, traffic):
    return pl.CostEstimate(flops=flops, bytes_accessed=traffic, transcendentals=0)


VMEM = pl.BlockSpec(memory_space=pltpu.VMEM)


def span_kernel(noise_ref, out_ref, band_ref):
    i = pl.program_id(0)

    @pl.when(i == 0)
    def _():
        shape = band_ref.shape
        index = lax.broadcasted_iota(jnp.int32, shape, 1) - lax.broadcasted_iota(jnp.int32, shape, 0) - 64 + FW
        band = jnp.zeros(shape, F32)
        for tap, value in enumerate(filter_taps().astype(np.float32)):
            band = jnp.where(index == tap, float(value), band)
        band_ref[...] = band.astype(BF16)

    windows = noise_ref.shape[2] // 128
    for w in range(windows):
        if w < windows - 1:
            window = noise_ref[0, :, 128 * w : 128 * w + 256]
        else:
            window = jnp.concatenate([noise_ref[0, :, 128 * w :], noise_ref[0, :, :128]], axis=-1)
        out_ref[i, 128 * w : 128 * w + 128] = lax.dot_general(
            band_ref[...], window, TURNED, preferred_element_type=F32
        ).astype(BF16)


def span_planes(noise):
    per, rows, length = noise.shape
    return pl.pallas_call(
        span_kernel,
        grid=(per,),
        in_specs=[pl.BlockSpec((1, rows, length), lambda i: (i, 0, 0))],
        out_specs=VMEM,
        out_shape=jax.ShapeDtypeStruct((per, length, rows), BF16),
        scratch_shapes=[pltpu.VMEM((128, 256), BF16)],
        compiler_params=pltpu.CompilerParams(vmem_limit_bytes=12 * 2**20),
        cost_estimate=cost(2 * 10**9, 4 * 10**6),
        name="span",
    )(noise)


ROUNDS = [(r, (d - r) % SIDE) for d in range(SIDE) for r in range(SIDE)]
SOON = 13


def seat():
    tile = lax.axis_index("tile")
    return lax.div(tile, 2 * SIDE), lax.rem(lax.div(tile, 2), SIDE), lax.rem(tile, 2), lax.axis_index("grp")


def rows_kernel(spans_ref, edges_ref, band_ref, own_ref, halo_ref, *refs):
    out_refs, done_ref = refs[:-1], refs[-1]
    per, length = spans_ref.shape[:2]
    windows, steps = 4, length // 512
    blocks = 2 * windows * steps
    band = band_ref[...]
    for step in range(steps):
        lo, hi = 512 * step, 512 * step + 640
        edges = edges_ref[:, lo:hi]
        if step == steps - 1:
            edges = jnp.concatenate([edges_ref[:, lo:], edges_ref[:, :128]], axis=-1)
        edge = jnp.concatenate(
            [
                lax.dot_general(
                    band, edges[:, 128 * v : 128 * v + 256], TURNED, preferred_element_type=F32
                ).astype(BF16)
                for v in range(windows)
            ],
            axis=0,
        )
        parts = [
            jnp.dot(spans_ref[i, lo : lo + 512], own_ref[i % 2], preferred_element_type=F32)
            + jnp.dot(edge, halo_ref[i], preferred_element_type=F32)
            for i in range(per)
        ]
        pairs = [part[:, :128] for part in parts]
        pairs += [parts[i][:, 128:] + parts[i + 1][:, 128:] for i in range(0, per, 2)]
        for k, pair in enumerate(pairs):
            pair = pair.astype(BF16)
            for v in range(2 * windows):
                done_ref[(2 * windows * step + 1 + v) % blocks, k] = pair[64 * v : 64 * (v + 1)]
    x, y, core, z = seat()
    for n, (r, d) in enumerate(ROUNDS):
        column = lax.rem(x - z + r + 2 * core + SIDE, SIDE)
        for h in range(2):
            target = (column * SIDE + lax.bitwise_xor(y, d)) * 2 + lax.rem(core + h, 2)
            out_refs[n][h] = done_ref[target]


def filter_rows(spans, halo, weights):
    block = (6, 64, 128)
    shapes = [(2,) + block] * len(ROUNDS)
    return pl.pallas_call(
        rows_kernel,
        in_specs=[VMEM] * 5,
        out_specs=[VMEM] * len(shapes),
        out_shape=[jax.ShapeDtypeStruct(a, BF16) for a in shapes],
        scratch_shapes=[pltpu.VMEM((4 * SIDE * 2,) + block, BF16)],
        compiler_params=pltpu.CompilerParams(vmem_limit_bytes=20 * 2**20),
        cost_estimate=cost(10**9, 4 * 10**6),
        name="rows",
    )(spans, halo, *weights)


def chain_kernel(*refs):
    count = len(ROUNDS)
    stay_refs, swap_refs = refs[:count], refs[count : count + 2]
    stress_ref, timescale_ref, mean_ref, courant_ref, prior_ref, field_ref = refs[count + 2 : count + 8]
    inflow_ref, result_ref, vel_ref, held_ref = refs[count + 8 :]
    groups, per = SIDE, 4
    depth = timescale_ref.shape[0]
    steps = groups * per
    low = lax.broadcasted_iota(jnp.int32, (depth, 128), 1) < 64
    x, y, core, z = seat()
    rows = pl.ds(pl.multiple_of(pl.program_id(0) * depth, depth), depth)
    for n, (r, d) in enumerate(ROUNDS):
        for h in range(2):
            came = lax.rem(core + h, 2)
            time = lax.rem(z - x + r + 2 * came + SIDE, SIDE)
            if h == 0:
                held_ref[came, time, d] = stay_refs[n][0, :, rows]
            else:
                held_ref[came, time, d] = swap_refs[0][n, :, rows] if n < SOON else swap_refs[1][n - SOON, :, rows]

    def band(d, _):
        lanes = pl.ds(pl.multiple_of(lax.bitwise_xor(y, d) * 128, 128), 128)
        courant = courant_ref[:, lanes]
        rest = 1.0 - courant
        inverse = 1.0 / rest
        decay = jnp.exp(-math.pi / (2.0 * timescale_ref[:, lanes]))
        gain = jnp.sqrt(1.0 - decay * decay)
        first = jnp.sqrt(stress_ref[0, :, lanes])
        second_low = stress_ref[1, :, lanes] / first
        second = jnp.sqrt(stress_ref[2, :, lanes] - second_low * second_low)
        third_low = stress_ref[3, :, lanes] / first
        third_mid = (stress_ref[4, :, lanes] - second_low * third_low) / second
        third = jnp.sqrt(stress_ref[5, :, lanes] - third_low * third_low - third_mid * third_mid)
        first, second_low, second = first * gain, second_low * gain, second * gain
        third_low, third_mid, third = third_low * gain, third_mid * gain, third * gain
        mean = mean_ref[:, lanes]
        phi = [prior_ref[m, :, lanes] / gain for m in range(3)]
        ratio = courant * inverse
        scale = ratio
        for g in range(groups):

            def pair(k):
                one, two = [held_ref[came, g, d, k].astype(F32) for came in range(2)]
                return jnp.where(low, one, pltpu.roll(two, 64, 1)), jnp.where(low, pltpu.roll(one, 64, 1), two)

            for half in range(2):
                third_planes = pair(4 + half)
                for i in range(2):
                    p = g * per + 2 * half + i
                    planes = (*pair(2 * half + i), third_planes[i])
                    phi = [decay * phi[m] + planes[m] for m in range(3)]
                    vel = (
                        mean + first * phi[0],
                        second_low * phi[0] + second * phi[1],
                        third_low * phi[0] + third_mid * phi[1] + third * phi[2],
                    )
                    for m in range(3):
                        inflow_ref[p, m, :, lanes] = vel[m].astype(BF16)
                        vel_ref[p, m] = vel[m] * scale
                    scale = scale * inverse
        back = rest / courant
        square = rest * rest
        square = square * square
        square = square * square
        last = square * square
        for m in range(3):
            power = None
            cells = []
            for j in range(CX):
                start = field_ref[m, j, :, lanes]
                cells.append(start if j == 0 else start * power)
                power = back if j == 0 else power * back
            for p in range(steps):
                inlet = vel_ref[p, m]
                cells = [cells[j] + (inlet if j == 0 else cells[j - 1]) for j in range(CX)]
            power = last
            for j in range(CX):
                result_ref[m, j, :, lanes] = cells[j] * power
                power = power * ratio
        return _

    lax.fori_loop(0, SIDE, band, 0)


def march_cells(stay, swap, stress, timescale, mean, courant, prior, field):
    rows = 16
    depth, length = timescale.shape
    steps = 16
    spec = lambda *lead: pl.BlockSpec(lead + (rows, length), lambda s: (0,) * len(lead) + (s, 0))
    return pl.pallas_call(
        chain_kernel,
        grid=(depth // rows,),
        in_specs=[VMEM] * (len(stay) + len(swap))
        + [spec(6), spec(), spec(), spec(), spec(3), spec(3, CX)],
        out_specs=[spec(steps, 3), spec(3, CX)],
        out_shape=[
            jax.ShapeDtypeStruct((steps, 3, depth, length), BF16),
            jax.ShapeDtypeStruct((3, CX, depth, length), F32),
        ],
        scratch_shapes=[
            pltpu.VMEM((steps, 3, rows, 128), F32),
            pltpu.VMEM((2, SIDE, SIDE, 6, rows, 128), BF16),
        ],
        compiler_params=pltpu.CompilerParams(vmem_limit_bytes=32 * 2**20),
        cost_estimate=cost(10**9, 14 * 10**6),
        name="march",
    )(*stay, *swap, stress, timescale, mean, courant, prior, field)


def place(x, y, core, z):
    return z * 32 + (x * SIDE + y) * 2 + core


def moves(target):
    seats = [(x, y, core, z) for x in range(SIDE) for y in range(SIDE) for core in range(2) for z in range(SIDE)]
    return [(place(*one), place(*target(*one))) for one in seats]


def exchange(blocks):
    got = []
    for block, (r, d) in zip(blocks, ROUNDS, strict=True):
        pairs = moves(lambda x, y, core, z: ((x - z + r + 2 * core) % SIDE, y ^ d, core, x))
        got.append(lax.ppermute(block, AXES, pairs))
    return got


def body(noise, stress, timescale, mean_inflow, courant, prior_state, field):
    per, comps, rows, length = noise.shape
    tiles = lax.axis_size("tile")
    flat = noise.reshape(per * comps, rows, length)
    up = [(i, i + 1) for i in range(tiles - 1)]
    down = [(i + 1, i) for i in range(tiles - 1)]
    before = lax.ppermute(flat[:, rows - FW :], "tile", up)
    after = lax.ppermute(flat[:, :FW], "tile", down)
    halo = jnp.concatenate([before, after], axis=1).reshape(per * comps * 2 * FW, length)
    weights = filter_weights(per, comps, rows)
    spans = span_planes(noise.reshape(per, comps * rows, length))
    other = moves(lambda x, y, core, z: (x, y, 1 - core, z))
    swap = []
    got = exchange(filter_rows(spans, halo, weights))
    for part in (got[:SOON], got[SOON:]):
        swap.append(lax.ppermute(jnp.stack([a[1] for a in part]), AXES, other))
    inflow, result = march_cells(got, swap, stress, timescale, mean_inflow, courant, prior_state, field)
    return (inflow, result)


def solution(mesh):
    placed = (
        P("grp", None, "tile", None),
        P(None, "tile", "grp"),
        P("tile", "grp"),
        P("tile", "grp"),
        P("tile", "grp"),
        P(None, "tile", "grp"),
        P(None, None, "tile", "grp"),
    )
    return jax.shard_map(
        body,
        mesh=mesh,
        in_specs=placed,
        out_specs=(P(None, None, "tile", "grp"), P(None, None, "tile", "grp")),
        check_vma=False,
    )
```
